128 devices in a mesh: group: 32 (over z, y, core), local: 4 (over x).
Axes of the slice: x: 4, y: 4, z: 4, core: 2. Of those that a mesh axis runs over, the one named last changes fastest.
Arguments:
- dense_vec: bfloat16 [16384, 128], P(('group', 'local')), may hold values from -6 to 6
- q_tables: float32 [4096, 26, 128], P('group'), may hold values from -4 to 4
- r_tables: float32 [256, 26, 128], P('local'), may hold values from -4 to 4
- owner: int32 [16384, 26, 1], P(('group', 'local')), may hold values from 0 to 31; in each aligned block of 3328 rows (0 to 3327, 3328 to 6655, ..., all dimensions but the last counted through in order) at most 208 rows name the same one
- q_local: int32 [16384, 26], P(('group', 'local')), may hold values from 0 to 127
- r_index: int32 [16384, 26], P(('group', 'local')), may hold values from 0 to 255
- w_one: bfloat16 [479, 1024], replicated, may hold values from -0.25 to 0.25
- b_one: float32 [1024], replicated, may hold values from -3 to 3
- w_two: bfloat16 [1024, 1024], replicated, may hold values from -0.1875 to 0.1875
- b_two: float32 [1024], replicated, may hold values from -3 to 3
- w_three: bfloat16 [1024, 512], replicated, may hold values from -0.1875 to 0.1875
- b_three: float32 [512], replicated, may hold values from -3 to 3
- w_four: bfloat16 [512, 256], replicated, may hold values from -0.25 to 0.25
- b_four: float32 [256], replicated, may hold values from -3 to 3
- cotangent: bfloat16 [16384, 256], P(('group', 'local')), may hold values from -6 to 6
Outputs:
- q_new: float32 [4096, 26, 128], P('group')
- r_new: float32 [256, 26, 128], P('local')
- w_one_new: float32 [479, 1024], replicated
- b_one_new: float32 [1024], replicated
- w_two_new: float32 [1024, 1024], replicated
- b_two_new: float32 [1024], replicated
- w_three_new: float32 [1024, 512], replicated
- b_three_new: float32 [512], replicated
- w_four_new: float32 [512, 256], replicated
- b_four_new: float32 [256], replicated
The draws below stay inside these ranges and needn't reach their ends.
Inputs may be any that keep to these rules, and one draw needn't show every extreme that they name: `owner`: within the rows of one device (its 128 samples times 26 tables), no group is named more than 208 times, a bound that some block reaches.
All inputs are finite; a program needn't handle non-finite values.
Results may differ from the reference program's by a relative error of at most 0.0025.
Values may be sent and summed in bfloat16 or wider, within the bound.
No kernel may reach another device: no remote copies, remote signals or barrier semaphores. Data moves between devices by JAX's collectives and lax.ppermute only.
A program may use at most 128 MiB of HBM per device.

```python
import math
import jax
import jax.numpy as jnp
import numpy as np
from jax import lax

TABLES = 26
DIM = 128
H1 = 1024
H2 = 1024
H3 = 512
H4 = 256
B_DEV = 128
QUOT_DEV = 128
FEAT = 479
BATCH = 16384
QUOT_ROWS = 4096
REM_ROWS = 256
CAP = 208
N_GROUP = 32
N_LOCAL = 4


def plant(result, own_key, least, largest):
    index_at = [jax.random.randint(jax.random.fold_in(own_key, axis), (), 0, length) for axis, length in enumerate(result.shape)]
    longest = result.shape.index(max(result.shape))
    beside = index_at[:longest] + [(index_at[longest] + 1) % result.shape[longest]] + index_at[longest + 1:]
    return result.at[tuple(index_at)].set(least).at[tuple(beside)].set(largest)


def levels(rng, extent, pieces, low, top_value):
    gain, own = 1.0, jax.random.fold_in(rng, 6)
    for position, parts in pieces:
        steps = jnp.exp(jax.random.uniform(jax.random.fold_in(own, position), (parts,), jnp.float32, low / len(pieces), top_value / len(pieces)))
        gain = gain * jnp.repeat(steps, extent[position] // parts).reshape([-1 if axis == position else 1 for axis in range(len(extent))])
    return gain


def rank_bounds(number_of, skew):
    loads = [(1 << 20) // math.isqrt(standing ** skew) + 1 for standing in range(1, number_of + 1)]
    deviation = 1 + sum(loads) // (1 << 30)
    return np.cumsum(np.array([max(1, weight // deviation) for weight in loads]))


def skewed_ids(own_key, dims, count, lean):
    listing = rank_bounds(count, lean)
    pick = jax.random.randint(jax.random.fold_in(own_key, 1), dims, 0, int(listing[count - 1]))
    grade = jnp.searchsorted(jnp.asarray(listing, jnp.int32), pick, side="right")
    return jax.random.permutation(jax.random.fold_in(own_key, 2), count)[grade].astype(jnp.int32)


def routed_block(stream_key, own, number, rows, amount, top, limit, lean):
    ranking = jax.random.permutation(stream_key, amount)
    packed, usual = portions_of(amount, rows * top, limit, lean, True), portions_of(amount, rows * top, limit, lean, False)
    places = jnp.arange(amount)

    def named(tallies, rotation):
        used = int((tallies > 0).sum())
        fixed = max(1, used // 4)
        passed = fixed + (places - fixed + rotation * (used - fixed)) % max(1, amount - fixed)
        return jnp.zeros((amount,), jnp.int32).at[ranking[jnp.where(places < fixed, places, passed)]].set(jnp.asarray(tallies, jnp.int32))

    tallies = jnp.where(number % 4 == 0, named(packed, number // 4), named(usual, number - number // 4 - 1))
    mixed = jax.random.permutation(jax.random.fold_in(own, 3), amount)
    source_of, receiver = mixed[0:amount // 2 * 2:2], mixed[1:amount // 2 * 2:2]
    slack = jnp.minimum(tallies[source_of] - 1, limit - tallies[receiver]) // 2
    slack = jnp.where((source_of == ranking[0]) | (receiver == ranking[0]) | (tallies[receiver] == 0), 0, jnp.maximum(slack, 0))
    passed = jax.random.randint(jax.random.fold_in(own, 4), (amount // 2,), 0, 1 << 20) % (slack + 1)
    tallies = tallies.at[source_of].add(-passed).at[receiver].add(passed)
    items = jnp.searchsorted(jnp.cumsum(tallies), jnp.arange(rows * top), side="right").astype(jnp.int32)
    table = items.reshape(top, rows).T
    table = table[jax.random.permutation(jax.random.fold_in(own, 1), rows)]
    rotation = jax.random.randint(jax.random.fold_in(own, 2), (rows, 1), 0, top)
    return jnp.take_along_axis(table, (jnp.arange(top)[None, :] + rotation) % top, axis=1)


def portions_of(number_of, total, reach, slope, full):
    loads = [(1 << 20) // math.isqrt(rank ** slope) + 1 for rank in range(1, number_of + 1)]
    largest = reach if full else min(reach, max(-(-total // number_of), total * loads[0] // sum(loads)))
    least = 1 if total - largest >= number_of - 1 else 0
    holding, surplus = [largest] + [least] * (number_of - 1), total - largest - least * (number_of - 1)
    while surplus > 0:
        free = [i for i in range(1, number_of) if holding[i] < largest] or [i for i in range(1, number_of) if holding[i] < reach]
        whole, left = sum([loads[i] for i in free]), surplus
        for i in free:
            more = min(reach - holding[i], max(1, left * loads[i] // whole), surplus)
            holding[i] = holding[i] + more
            surplus = surplus - more
    return np.array(holding)


def centred(stream_key, extent, scale, reach, pieces=(), held_as=jnp.bfloat16):
    factor_of = levels(stream_key, extent, pieces, -0.22, 0.18) if pieces else 1.0
    result = jax.random.normal(stream_key, extent, jnp.float32) * scale * factor_of
    return jnp.minimum(jnp.maximum(result, -reach), reach).astype(held_as)


def setup_inputs(seed: int = 0) -> dict:
    streams_of = jax.random.split(jax.random.key(seed), 16)
    dense_vec = centred(streams_of[0], (BATCH, DIM), 1.0, 6.0, ((0, 128),))
    q_tables = centred(streams_of[1], (QUOT_ROWS, TABLES, DIM), 0.5, 4.0, ((0, 32),), jnp.float32)
    r_tables = centred(streams_of[2], (REM_ROWS, TABLES, DIM), 0.5, 4.0, ((0, 4),), jnp.float32)
    owner_keys = jax.random.split(jax.random.fold_in(streams_of[3], 1), BATCH * TABLES // (B_DEV * TABLES))
    owner_turns = jax.random.permutation(jax.random.fold_in(streams_of[3], 3), BATCH * TABLES // (B_DEV * TABLES))
    owner = jax.vmap(lambda own, number: routed_block(jax.random.fold_in(streams_of[3], 2), own, number, B_DEV * TABLES, N_GROUP, 1, CAP, 2))(owner_keys, owner_turns).reshape((BATCH, TABLES, 1))
    q_local = plant(skewed_ids(streams_of[4], (BATCH, TABLES), QUOT_DEV, 2), jax.random.fold_in(streams_of[4], 3), 0, QUOT_DEV - 1).astype(jnp.int32)
    r_index = plant(jax.random.randint(streams_of[5], (BATCH, TABLES), 0, REM_ROWS), jax.random.fold_in(streams_of[5], 1), 0, REM_ROWS - 1).astype(jnp.int32)
    w_one = centred(streams_of[6], (FEAT, H1), FEAT ** -0.5, 0.25)
    b_one = centred(streams_of[7], (H1,), 0.5, 3.0, (), jnp.float32)
    w_two = centred(streams_of[8], (H1, H2), H1 ** -0.5, 0.1875)
    b_two = centred(streams_of[9], (H2,), 0.5, 3.0, (), jnp.float32)
    w_three = centred(streams_of[10], (H2, H3), H2 ** -0.5, 0.1875)
    b_three = centred(streams_of[11], (H3,), 0.5, 3.0, (), jnp.float32)
    w_four = centred(streams_of[12], (H3, H4), H3 ** -0.5, 0.25)
    b_four = centred(streams_of[13], (H4,), 0.5, 3.0, (), jnp.float32)
    cotangent = centred(streams_of[14], (BATCH, H4), 1.0, 6.0, ((0, 128),))
    return dict(dense_vec=dense_vec, q_tables=q_tables, r_tables=r_tables, owner=owner, q_local=q_local, r_index=r_index, w_one=w_one, b_one=b_one, w_two=w_two, b_two=b_two, w_three=w_three, b_three=b_three, w_four=w_four, b_four=b_four, cotangent=cotangent)


table_rate = 0.05
dense_rate = 0.0005


def silu_slope(preact):
    sigma = jax.nn.sigmoid(preact)
    return sigma * (1.0 + preact * (1.0 - sigma))


def interact(dense_rows, embeds):
    vectors_all = jnp.concatenate([dense_rows[:, None, :], embeds], axis=1).astype(jnp.float32)
    gram_mat = jnp.einsum("bid,bjd->bij", vectors_all, vectors_all, precision=lax.Precision.HIGHEST)
    lower_i, lower_j = np.tril_indices(vectors_all.shape[1], -1)
    pair_vals = gram_mat[:, lower_i, lower_j]
    features = jnp.concatenate([dense_rows.astype(jnp.float32), pair_vals], axis=1).astype(jnp.bfloat16)
    return vectors_all, features


def pair_back(d_pairs, vectors_all):
    vectors = vectors_all.shape[1]
    lower_i, lower_j = np.tril_indices(vectors, -1)
    spread = jnp.zeros((vectors_all.shape[0], vectors, vectors), jnp.float32).at[:, lower_i, lower_j].set(d_pairs)
    spread = spread + jnp.swapaxes(spread, 1, 2)
    return jnp.einsum("bij,bjd->bid", spread, vectors_all, precision=lax.Precision.HIGHEST)


def contract_rows(left, right):
    return lax.dot_general(left, right, (((0,), (0,)), ((), ())), preferred_element_type=jnp.float32)


def dense_pass(features, layers, cot_rows):
    inputs_list = [features]
    pre_list = []
    current = features
    for layer_idx, (weight, biases) in enumerate(layers):
        pre_act = jnp.dot(current, weight, preferred_element_type=jnp.float32) + biases
        pre_list.append(pre_act)
        if layer_idx + 1 < len(layers):
            current = jax.nn.silu(pre_act).astype(jnp.bfloat16)
            inputs_list.append(current)
    grad_low = cot_rows
    grad_full = cot_rows.astype(jnp.float32)
    grads = []
    back_grad = None
    for layer_idx in reversed(range(len(layers))):
        weight = layers[layer_idx][0]
        w_grad = contract_rows(inputs_list[layer_idx], grad_low)
        b_grad = jnp.sum(grad_full, axis=0)
        back_grad = lax.dot_general(grad_low, weight, (((1,), (1,)), ((), ())), preferred_element_type=jnp.float32)
        grads.insert(0, (w_grad, b_grad))
        if layer_idx > 0:
            grad_full = back_grad * silu_slope(pre_list[layer_idx - 1])
            grad_low = grad_full.astype(jnp.bfloat16)
    return grads, back_grad


def reference(dense_vec, q_tables, r_tables, owner, q_local, r_index, w_one, b_one, w_two, b_two, w_three, b_three, w_four, b_four, cotangent):
    layers = [(w_one, b_one), (w_two, b_two), (w_three, b_three), (w_four, b_four)]
    block = B_DEV * N_LOCAL
    block_count = BATCH // block
    table_ids = jnp.arange(TABLES, dtype=jnp.int32)[None, :]
    q_flat_table = q_tables.reshape(QUOT_ROWS * TABLES, DIM)
    r_flat_table = r_tables.reshape(REM_ROWS * TABLES, DIM)
    owner_all = owner[:, :, 0]

    def block_step(totals, offset):
        q_grad, r_grad, dense_grads = totals
        dense_rows = lax.dynamic_slice_in_dim(dense_vec, offset, block, 0)
        owner_rows = lax.dynamic_slice_in_dim(owner_all, offset, block, 0)
        local_rows = lax.dynamic_slice_in_dim(q_local, offset, block, 0)
        rem_rows = lax.dynamic_slice_in_dim(r_index, offset, block, 0)
        cot_rows = lax.dynamic_slice_in_dim(cotangent, offset, block, 0)
        q_flat = ((owner_rows * QUOT_DEV + local_rows) * TABLES + table_ids).reshape(-1).astype(jnp.int32)
        r_flat = (rem_rows * TABLES + table_ids).reshape(-1).astype(jnp.int32)
        q_rows = q_flat_table[q_flat].astype(jnp.bfloat16)
        r_rows = r_flat_table[r_flat]
        q_val = q_rows.astype(jnp.float32)
        embeds = (q_val * r_rows).astype(jnp.bfloat16).reshape(block, TABLES, DIM)
        vectors_all, features = interact(dense_rows, embeds)
        grads, d_features = dense_pass(features, layers, cot_rows)
        d_embed = pair_back(d_features[:, DIM:], vectors_all)[:, 1:, :].reshape(-1, DIM)
        q_grad = q_grad.at[q_flat].add(d_embed * r_rows)
        r_grad = r_grad.at[r_flat].add(d_embed * q_val)
        dense_grads = jax.tree.map(jnp.add, dense_grads, grads)
        return (q_grad, r_grad, dense_grads), None

    start_grads = [(jnp.zeros(weight.shape, jnp.float32), jnp.zeros(biases.shape, jnp.float32)) for weight, biases in layers]
    start_totals = (jnp.zeros((QUOT_ROWS * TABLES, DIM), jnp.float32), jnp.zeros((REM_ROWS * TABLES, DIM), jnp.float32), start_grads)
    offsets = jnp.arange(block_count, dtype=jnp.int32) * block
    (q_grad, r_grad, dense_grads), unused = lax.scan(block_step, start_totals, offsets)
    q_new = q_tables - table_rate * q_grad.reshape(q_tables.shape)
    r_new = r_tables - table_rate * r_grad.reshape(r_tables.shape)
    updated = []
    for (weight, biases), (w_grad, b_grad) in zip(layers, dense_grads):
        updated.append(weight.astype(jnp.float32) - dense_rate * w_grad)
        updated.append(biases - dense_rate * b_grad)
    return (q_new, r_new, updated[0], updated[1], updated[2], updated[3], updated[4], updated[5], updated[6], updated[7])
```

```python
import jax
import jax.numpy as jnp
import numpy as np
from jax import lax
from jax.experimental import pallas as pl
from jax.experimental.pallas import tpu as pltpu
from jax.sharding import PartitionSpec as P

table_rate = 0.05
dense_rate = 0.0005
BF = jnp.bfloat16
F32 = jnp.float32
I32 = jnp.int32

GROUPS = 32
LOCALS = 4
TABLES = 26
ROWS = 128
DIM = 128
CAP = 208
LOOKUPS = TABLES * ROWS
SLOTS = GROUPS * CAP
FEAT = 479
PAIRS = 351
REM = 256
BOTH = ("group", "local")
CORE_PAIRS = [[2 * i, 2 * i + 1] for i in range(GROUPS // 2)]
SAME_CORE = [list(range(c, GROUPS, 2)) for c in range(2)]
SAME_CORE_ALL = [
    [g * LOCALS + l for g in range(c, GROUPS, 2) for l in range(LOCALS)] for c in range(2)
]
VMEM_LIMIT = 20 * 1024 * 1024


def smem():
    return pl.BlockSpec(memory_space=pltpu.SMEM)


def vmem():
    return pl.BlockSpec(memory_space=pltpu.VMEM)


def call(kernel, out, in_specs, scratch, name):
    return pl.pallas_call(
        kernel,
        out_shape=out,
        in_specs=in_specs,
        out_specs=vmem(),
        scratch_shapes=scratch,
        compiler_params=pltpu.CompilerParams(vmem_limit_bytes=VMEM_LIMIT),
        name=name,
    )


def serve_kernel(keys, table, out, rows):
    def step(g, carry):
        for c in range(CAP):
            rows[c : c + 1, :] = table[pl.ds(keys[g, c], 1), :]
        out[g] = rows[...].astype(BF)
        return carry

    lax.fori_loop(0, GROUPS, step, 0)


def serve(keys, table):
    return call(
        serve_kernel,
        jax.ShapeDtypeStruct((GROUPS, CAP, DIM), BF),
        [smem(), vmem()],
        [pltpu.VMEM((CAP, DIM), F32)],
        "serve_rows",
    )(keys, table)


ALL_PAIRS = 384
IDS = 32
BLOCK = 256
NEXT = 28 * IDS


def sigma_of(preact):
    sigma = jax.nn.sigmoid(preact)
    return (preact * sigma).astype(BF), sigma * (1.0 + preact * (1.0 - sigma))


def times(left, right):
    return jnp.dot(left, right, preferred_element_type=F32)


def times_turned(left, right):
    return lax.dot_general(left, right, (((1,), (1,)), ((), ())), preferred_element_type=F32)


def every(first):
    return pl.ds(first, ROWS, stride=IDS)


def compute_kernel(
    position,
    arrived,
    r_rows,
    dense,
    w_one,
    b_one,
    w_two,
    b_two,
    w_three,
    b_three,
    w_four,
    cot,
    select,
    mirror,
    outbound,
    feats,
    act_one,
    act_two,
    act_three,
    grad_one,
    grad_two,
    grad_three,
    d_low,
    sums,
    wide,
    rows,
    q_rows,
    tall,
    low,
    mixed,
):
    def group_rows(g):
        return pl.ds(pl.multiple_of(g * CAP, 16), CAP)

    def widen(g, carry):
        wide[group_rows(g), :] = arrived[g].astype(F32)
        return carry

    lax.fori_loop(0, GROUPS, widen, 0)
    tall[every(0), :] = dense[...].astype(F32)
    for i in range(TABLES + 1, IDS):
        tall[every(i), :] = jnp.zeros((ROWS, DIM), F32)

    def embed(t, carry):
        for b in range(ROWS):
            rows[b : b + 1, :] = wide[pl.ds(position[t, b], 1), :]
        values = rows[...]
        q_rows[t] = values
        tall[every(t + 1), :] = (values * r_rows[t]).astype(BF).astype(F32)
        return carry

    lax.fori_loop(0, TABLES, embed, 0)

    row_id = lax.broadcasted_iota(I32, (BLOCK, BLOCK), 0)
    lane_id = lax.broadcasted_iota(I32, (BLOCK, BLOCK), 1)
    same = (row_id // IDS) == (lane_id // IDS)
    row_id = lax.broadcasted_iota(I32, (BLOCK, DIM), 0)
    lane_id = lax.broadcasted_iota(I32, (BLOCK, DIM), 1)
    fold = ((row_id % IDS) == (lane_id % IDS)).astype(BF)
    quarter = (row_id % 4) == (lane_id // IDS)

    def block(n):
        return pl.ds(pl.multiple_of(n * BLOCK, BLOCK), BLOCK)

    def gram(n, carry):
        own = tall[block(n), :].astype(BF)
        low[block(n), :] = own
        products = jnp.where(same, times_turned(own, own), 0.0).astype(BF)
        mixed[block(n), :] = jnp.where(quarter, times(products, fold), 0.0)
        return carry

    lax.fori_loop(0, ROWS * IDS // BLOCK, gram, 0)
    grams = []
    for m in range(7):
        part = mixed[every(4 * m), :]
        for k in range(1, 4):
            part = part + mixed[every(4 * m + k), :]
        grams.append(part.astype(BF))
    pairs = times(jnp.concatenate(grams, axis=1), select[...])
    lane = lax.broadcasted_iota(I32, (ROWS, ALL_PAIRS), 1)
    pairs = jnp.where(lane == PAIRS, 1.0, pairs)
    feats[:, :DIM] = dense[...]
    feats[:, DIM:] = pairs.astype(BF)

    act, slope_one = sigma_of(times(feats[...], w_one[...]) + b_one[...])
    act_one[...] = act
    act, slope_two = sigma_of(times(act, w_two[...]) + b_two[...])
    act_two[...] = act
    act, slope_three = sigma_of(times(act, w_three[...]) + b_three[...])
    act_three[...] = act

    full = times_turned(cot[...], w_four[...]) * slope_three
    sums[...] = jnp.zeros((8, 1024), F32)
    sums[1:2, :512] = jnp.sum(full, axis=0, keepdims=True)
    sums[1:2, 512:768] = jnp.sum(cot[...].astype(F32), axis=0, keepdims=True)
    grad = full.astype(BF)
    grad_three[...] = grad
    full = times_turned(grad, w_three[...]) * slope_two
    sums[0:1, :] = jnp.sum(full, axis=0, keepdims=True)
    grad = full.astype(BF)
    grad_two[...] = grad
    grad = (times_turned(grad, w_two[...]) * slope_one).astype(BF)
    grad_one[...] = grad
    d_pairs = times_turned(grad, w_one[DIM:, :])
    high = d_pairs.astype(BF)
    spread = times(high, mirror[...])
    lane = lax.broadcasted_iota(I32, (ROWS, DIM), 1) // IDS
    for m in range(7):
        part = spread[:, m * DIM : (m + 1) * DIM]
        for k in range(4):
            mixed[every(4 * m + k), :] = jnp.where(lane == k, part, 0.0)

    def back(n, carry):
        unfolded = times_turned(mixed[block(n), :].astype(BF), fold)
        unfolded = jnp.where(same, unfolded, 0.0).astype(BF)
        tall[block(n), :] = times(unfolded, low[block(n), :])
        return carry

    lax.fori_loop(0, ROWS * IDS // BLOCK, back, 0)

    def clear(g, carry):
        wide[group_rows(g), :] = jnp.zeros((CAP, DIM), F32)
        return carry

    lax.fori_loop(0, GROUPS, clear, 0)

    def route(t, carry):
        d_embed = tall[every(t + 1), :]
        d_low[t] = (d_embed * q_rows[t]).astype(BF)
        rows[...] = d_embed * r_rows[t]
        for b in range(ROWS):
            wide[pl.ds(position[t, b], 1), :] = rows[b : b + 1, :]
        return carry

    lax.fori_loop(0, TABLES, route, 0)

    def narrow(g, carry):
        outbound[g] = wide[group_rows(g), :].astype(BF)
        return carry

    lax.fori_loop(0, GROUPS, narrow, 0)


def compute(position, *arrays):
    shape = jax.ShapeDtypeStruct
    return pl.pallas_call(
        compute_kernel,
        out_shape=(
            shape((GROUPS, CAP, DIM), BF),
            shape((ROWS, DIM + ALL_PAIRS), BF),
            shape((ROWS, 1024), BF),
            shape((ROWS, 1024), BF),
            shape((ROWS, 512), BF),
            shape((ROWS, 1024), BF),
            shape((ROWS, 1024), BF),
            shape((ROWS, 512), BF),
            shape((TABLES, ROWS, DIM), BF),
            shape((8, 1024), F32),
        ),
        in_specs=[smem()] + [vmem()] * len(arrays),
        out_specs=(vmem(),) * 10,
        scratch_shapes=[
            pltpu.VMEM((SLOTS, DIM), F32),
            pltpu.VMEM((ROWS, DIM), F32),
            pltpu.VMEM((TABLES, ROWS, DIM), F32),
            pltpu.VMEM((ROWS * IDS, DIM), F32),
            pltpu.VMEM((ROWS * IDS, DIM), BF),
            pltpu.VMEM((ROWS * IDS, DIM), F32),
        ],
        compiler_params=pltpu.CompilerParams(vmem_limit_bytes=40 * 1024 * 1024),
        name="compute_step",
    )(position, *arrays)


DENSE_LANES = 2176
R_LANES = 7 * DIM
PACKED = DENSE_LANES + R_LANES
HALF_TABLES = 14


def weight_kernel(
    feats, act_one, act_two, act_three, grad_one, grad_two, grad_three, cot, d_low, r_row, sums, out
):
    def contract(left, first, right):
        return lax.dot_general(
            left[:, first : first + BLOCK],
            right,
            (((0,), (0,)), ((), ())),
            preferred_element_type=F32,
        ).astype(BF)

    for first in range(0, 1024, BLOCK):
        out[first : first + BLOCK, :1024] = contract(act_one, first, grad_two[...])
        out[first : first + BLOCK, 1024:1536] = contract(act_two, first, grad_three[...])
    for first in range(0, 512, BLOCK):
        for half in range(2):
            out[half * 512 + first : half * 512 + first + BLOCK, 1536:2048] = contract(
                feats, first, grad_one[:, half * 512 : half * 512 + 512]
            )
            out[half * 512 + first : half * 512 + first + BLOCK, 2048:2176] = contract(
                act_three, first, cot[:, half * DIM : half * DIM + DIM]
            )
    row = lax.broadcasted_iota(I32, (32, 512), 0)
    for half in range(2):
        at = slice(half * 512, half * 512 + 512)
        tail = jnp.where(
            row == 0, sums[0:1, at], jnp.where(row == 1, sums[1:2, at], jnp.zeros((32, 512), F32))
        )
        out[half * 512 + 480 : half * 512 + 512, 1536:2048] = tail.astype(BF)

    rem = lax.broadcasted_iota(I32, (REM, ROWS), 0)
    for t in range(2 * HALF_TABLES):
        core, within = divmod(t, HALF_TABLES)
        if t < TABLES:
            pick = (rem == r_row[t]).astype(BF)
            part = times(pick, d_low[t]).astype(BF)
        else:
            part = jnp.zeros((REM, DIM), BF)
        for l in range(LOCALS):
            for j in range(8):
                zy, k = divmod(within * 8 + j, 7)
                top = core * 512 + (zy * LOCALS + l) * 8
                left = DENSE_LANES + k * DIM
                first = l * 64 + j * 8
                out[top : top + 8, left : left + DIM] = part[first : first + 8, :]


def weight_grads(*arrays):
    return call(
        weight_kernel,
        jax.ShapeDtypeStruct((1024, PACKED), BF),
        [vmem()] * len(arrays),
        [],
        "weight_grads",
    )(*arrays)


LANES = 4
CHUNK = 16


def segment_kernel(keys, returned, out, wide, *sums):
    def widen(g, carry):
        wide[pl.ds(pl.multiple_of(g * CAP, 16), CAP), :] = returned[g].astype(F32)
        return carry

    lax.fori_loop(0, GROUPS, widen, 0)

    def clear(t, carry):
        at = pl.ds(pl.multiple_of(t * ROWS, 16), ROWS)
        for part in sums:
            part[at, :] = jnp.zeros((ROWS, DIM), F32)
        return carry

    lax.fori_loop(0, TABLES, clear, 0)
    share = GROUPS // LANES

    def step(i, carry):
        inner = i // (CAP // CHUNK)
        first = pl.multiple_of((i % (CAP // CHUNK)) * CHUNK, CHUNK)
        for c in range(CHUNK):
            for k in range(LANES):
                g = k * share + inner
                at = pl.ds(keys[g, first + c], 1)
                sums[k][at, :] = sums[k][at, :] + wide[pl.ds(g * CAP + first + c, 1), :]
        return carry

    lax.fori_loop(0, share * (CAP // CHUNK), step, 0)

    def finish(t, carry):
        at = pl.ds(pl.multiple_of(t * ROWS, 16), ROWS)
        total = sums[0][at, :]
        for part in sums[1:]:
            total = total + part[at, :]
        out[at, :] = total.astype(BF)
        return carry

    lax.fori_loop(0, TABLES, finish, 0)


def segment_rows(keys, returned):
    return call(
        segment_kernel,
        jax.ShapeDtypeStruct((LOOKUPS, DIM), BF),
        [smem(), vmem()],
        [pltpu.VMEM((SLOTS, DIM), F32)] + [pltpu.VMEM((LOOKUPS, DIM), F32)] * LANES,
        "segment_rows",
    )(keys, returned)


def pair_columns():
    vectors = TABLES + 1
    lower = np.full((28, IDS), -1, np.int32)
    lower_i, lower_j = np.tril_indices(vectors, -1)
    lower[lower_i, lower_j] = np.arange(PAIRS)
    both = lower.copy()
    both[lower_j, lower_i] = np.arange(PAIRS)
    return (lower.reshape(NEXT), both.reshape(NEXT))


def summed(blocks):
    return blocks.astype(F32).sum(axis=0).astype(BF)


def pair_summed(blocks):
    return summed(
        lax.all_to_all(blocks, "group", 0, 0, tiled=True, axis_index_groups=CORE_PAIRS)
    )


def pair_gathered(block):
    return lax.all_to_all(
        jnp.broadcast_to(block[None], (2, *block.shape)),
        "group",
        0,
        0,
        tiled=True,
        axis_index_groups=CORE_PAIRS,
    )


def body(
    dense_vec,
    q_tables,
    r_tables,
    owner,
    q_local,
    r_index,
    w_one,
    b_one,
    w_two,
    b_two,
    w_three,
    b_three,
    w_four,
    b_four,
    cotangent,
):
    dest = owner[:, :, 0].T
    q_row = q_local.T
    r_row = r_index.T
    hits = (dest[:, :, None] == jnp.arange(GROUPS, dtype=I32)).astype(BF)
    earlier = (jnp.arange(ROWS)[:, None] > jnp.arange(ROWS)[None, :]).astype(BF)
    within = jnp.einsum("cb,tbg->tcg", earlier, hits, preferred_element_type=F32)
    counts = jnp.sum(hits.astype(F32), axis=1)
    tables_before = (jnp.arange(TABLES)[:, None] > jnp.arange(TABLES)[None, :]).astype(F32)
    before = jnp.dot(tables_before, counts, precision=lax.Precision.HIGHEST)
    rank = jnp.sum((within + before[:, None, :]) * hits.astype(F32), axis=2).astype(I32)
    position = dest * CAP + rank
    ranks = (rank[:, :, None] == jnp.arange(CAP, dtype=I32)).astype(BF)
    table_ids = jnp.arange(TABLES, dtype=I32)[:, None, None].astype(BF)
    tagged = jnp.concatenate([hits * q_row[:, :, None].astype(BF), hits * table_ids], axis=2)
    slots = jnp.einsum("tbg,tbc->gc", tagged, ranks, preferred_element_type=F32).astype(I32)
    outgoing = slots[GROUPS:] * ROWS + slots[:GROUPS]

    request = lax.all_to_all(outgoing, "group", 0, 0, tiled=True)
    table_rows = jnp.swapaxes(q_tables, 0, 1).reshape(LOOKUPS, DIM)
    served = serve(request, table_rows)
    arrived = lax.all_to_all(served, "group", 0, 0, tiled=True)

    full_r = lax.all_gather(r_tables, "local", axis=0, tiled=True)
    r_pick = (r_row[:, :, None] == jnp.arange(REM, dtype=I32)).astype(BF)
    r_high = lax.reduce_precision(full_r, 8, 7)
    r_low = full_r - r_high
    r_rows = jnp.einsum(
        "tbr,rtd->tbd", r_pick, r_high.astype(BF), preferred_element_type=F32
    ) + jnp.einsum("tbr,rtd->tbd", r_pick, r_low.astype(BF), preferred_element_type=F32)

    lower, both = pair_columns()
    columns = jnp.arange(ALL_PAIRS, dtype=I32)
    select = (jnp.asarray(lower)[:, None] == columns[None, :]).astype(BF)
    mirror = (jnp.asarray(both)[None, :] == columns[:, None]).astype(BF)
    w_padded = jnp.pad(w_one, ((0, 33), (0, 0)))
    arrived, r_rows, select, mirror, w_padded, table_rows = lax.optimization_barrier(
        (arrived, r_rows, select, mirror, w_padded, table_rows)
    )
    outbound, *saved, d_low, sums = compute(
        position,
        arrived,
        r_rows,
        dense_vec,
        w_padded,
        b_one[None],
        w_two,
        b_two[None],
        w_three,
        b_three[None],
        w_four,
        cotangent,
        select,
        mirror,
    )
    returned = lax.all_to_all(outbound, "group", 0, 0, tiled=True)

    packed = weight_grads(*saved, cotangent, d_low, r_row[:, None, :], sums)
    half = pair_summed(packed.reshape(2, 512, PACKED)).reshape(2 * GROUPS, 8, PACKED)
    own = summed(
        lax.all_to_all(half, BOTH, 0, 0, tiled=True, axis_index_groups=SAME_CORE_ALL)
    )
    w_half = lax.all_to_all(
        jnp.broadcast_to(own[None, :, :DENSE_LANES], (2 * GROUPS, 8, DENSE_LANES)),
        BOTH,
        0,
        0,
        tiled=True,
        axis_index_groups=SAME_CORE_ALL,
    ).reshape(512, DENSE_LANES)
    w_all = pair_gathered(w_half).reshape(1024, DENSE_LANES)
    r_half = lax.all_to_all(
        jnp.broadcast_to(own[None, :, DENSE_LANES:], (GROUPS // 2, 8, R_LANES)),
        "group",
        0,
        0,
        tiled=True,
        axis_index_groups=SAME_CORE,
    )
    r_grad = pair_gathered(r_half).reshape(2, GROUPS // 2, 8, 7, DIM)
    r_grad = jnp.swapaxes(r_grad, 2, 3).reshape(28, 64, DIM)[:TABLES]
    r_new = r_tables - table_rate * jnp.swapaxes(r_grad, 0, 1).astype(F32)

    q_part = segment_rows(request, returned)
    q_piece = summed(
        lax.all_to_all(q_part.reshape(LOCALS, LOOKUPS // LOCALS, DIM), "local", 0, 0, tiled=True)
    )
    q_grad = lax.all_gather(q_piece, "local", axis=0, tiled=True).reshape(TABLES, ROWS, DIM)
    q_new = q_tables - table_rate * jnp.swapaxes(q_grad, 0, 1).astype(F32)

    first = w_all[:, 1536:2048]
    first = jnp.concatenate([first[:512], first[512:]], axis=1).astype(F32)
    last = w_all[:, 2048:]
    last = jnp.concatenate([last[:512], last[512:]], axis=1).astype(F32)
    return (
        q_new,
        r_new,
        w_one.astype(F32) - dense_rate * first[:FEAT],
        b_one - dense_rate * first[FEAT],
        w_two.astype(F32) - dense_rate * w_all[:, :1024].astype(F32),
        b_two - dense_rate * first[FEAT + 1],
        w_three.astype(F32) - dense_rate * w_all[:, 1024:1536].astype(F32),
        b_three - dense_rate * first[FEAT + 2, :512],
        w_four.astype(F32) - dense_rate * last,
        b_four - dense_rate * first[FEAT + 2, 512:768],
    )


def solution(mesh):
    rows = P(("group", "local"), None)
    return jax.shard_map(
        body,
        mesh=mesh,
        in_specs=(
            rows,
            P("group", None, None),
            P("local", None, None),
            P(("group", "local"), None, None),
            rows,
            rows,
            P(),
            P(),
            P(),
            P(),
            P(),
            P(),
            P(),
            P(),
            rows,
        ),
        out_specs=(
            P("group", None, None),
            P("local", None, None),
            P(),
            P(),
            P(),
            P(),
            P(),
            P(),
            P(),
            P(),
        ),
        check_vma=False,
    )
```
